32 devices in a mesh: groups: 2 (over x), pts: 8 (over z, y), lm: 2 (over core).
Axes of the slice: x: 2, y: 2, z: 4, core: 2. Of those that a mesh axis runs over, the one named last changes fastest.
Arguments:
- points: float32 [3, 4096], P(None, ('groups', 'pts', 'lm')), parts along dimension 1, may hold values from 0 to 1, as said below
- targets: float32 [32, 4096], P(None, ('groups', 'pts', 'lm')), parts along dimension 1, may hold values from -12 to 12
- order: int32 [4096], P(('groups', 'pts', 'lm')), parts along dimension 0, may hold values from 0 to 2047, as said below
- landmarks: int32 [2048], P('groups'), parts along dimension 0, may hold values from 0 to 2047, as said below
Outputs:
- coefficients: float32 [32, 4096], P(None, ('groups', 'pts', 'lm')), parts along dimension 1
- residual: float32 [32, 4096], P(None, ('groups', 'pts', 'lm')), parts along dimension 1
The draws below stay inside these ranges and needn't reach their ends.
There are 2 independent parts, one for each index of `groups`. The reference program is written for one: setup_inputs(seed, part) draws one part's arguments, and reference() takes and returns one part's arrays. A program takes and returns all parts, laid end to end along the dimension named above; each array names one. Nothing has to cross between parts.
Inputs may be any that keep to these rules, and one draw needn't show every extreme that they name: Each column is a point of the unit cube. Points are stored in Z-order: the 128 points of each aligned block of columns lie in one box of a regular grid, and consecutive blocks follow the Z-order curve through the boxes. `order`: A permutation of 0 to 2047. `landmarks`: 1024 distinct point indices.
All inputs are finite; a program needn't handle non-finite values.
Results may differ from the reference program's by a relative error of at most 0.0003.
Values sent between devices are 32-bit elements; how exact they have to be, the bound alone decides.
No kernel may reach another device: no remote copies, remote signals or barrier semaphores. Data moves between devices by JAX's collectives and lax.ppermute only.
A program may use at most 128 MiB of HBM per device.

```python
import math
import jax
import jax.numpy as jnp
from jax import lax

LANDMARKS = 1024
RHS = 32
ROWS_DEV = 128
ITERS = 2
POINTS = 2048


def shuffled(key):
    return jax.random.permutation(jax.random.fold_in(key, 11), POINTS).astype(jnp.int32)


def scattered(key):
    index = jnp.arange(POINTS, dtype=jnp.int32) // ROWS_DEV
    blocks = POINTS // ROWS_DEV
    levels = max(blocks - 1, 1).bit_length()
    corner = [jnp.zeros((POINTS,), jnp.float32) for axis in range(3)]
    sides = [1, 1, 1]
    for level in range(levels):
        axis = level % 3
        digit = index // 2 ** level % 2
        corner[axis] = corner[axis] + digit.astype(jnp.float32) * sides[axis]
        sides[axis] = sides[axis] * 2
    jitter = jax.random.uniform(jax.random.fold_in(key, 7), (3, POINTS), jnp.float32)
    return jnp.stack([(corner[axis] + jitter[axis]) / sides[axis] for axis in range(3)])


def draw_points(key, part):
    return scattered(key)


def draw_order(key, part):
    return shuffled(key)


def draw_landmarks(key, part):
    chosen = jax.random.permutation(jax.random.fold_in(key, 23), POINTS)
    return chosen[:LANDMARKS].astype(jnp.int32)


def draw_targets(key, part):
    order = shuffled(key)
    rank = jnp.zeros((POINTS,), jnp.int32).at[order].set(jnp.arange(POINTS, dtype=jnp.int32))
    spread = 0.3 * jnp.exp(jnp.log(10.0) * rank.astype(jnp.float32) / max(POINTS - 1, 1))
    noise_key = jax.random.fold_in(key, 31)
    return spread[None, :] * jnp.clip(jax.random.normal(noise_key, (RHS, POINTS), jnp.float32), -4.0, 4.0)


def setup_inputs(seed: int = 0, part: int = 0) -> dict:
    keys = jax.random.split(jax.random.key(seed), 5)
    own_keys = jax.random.split(jax.random.fold_in(keys[4], part), 5)
    points = draw_points(jax.random.fold_in(jax.random.fold_in(keys[4], part), 71), part)
    targets = draw_targets(jax.random.fold_in(jax.random.fold_in(keys[4], part), 71), part)
    order = draw_order(jax.random.fold_in(jax.random.fold_in(keys[4], part), 71), part)
    landmarks = draw_landmarks(jax.random.fold_in(jax.random.fold_in(keys[4], part), 71), part)
    return {"points": points, "targets": targets, "order": order, "landmarks": landmarks}


root_five = 2.23606797749979
signal_var = 0.1
inverse_square_length = 25.0
highest = lax.Precision.HIGHEST

def matern(near, far):
    first = near[0][:, None] - far[0][None, :]
    second = near[1][:, None] - far[1][None, :]
    third = near[2][:, None] - far[2][None, :]
    scaled = (first * first + second * second + third * third) * inverse_square_length
    reach = jnp.sqrt(scaled)
    return signal_var * (1.0 + root_five * reach + 5.0 / 3.0 * scaled) * jnp.exp(-root_five * reach)

def operator(points, vector):
    total = points.shape[1]
    block = math.gcd(total, 256)

    def rows_block(index):
        near = lax.dynamic_slice_in_dim(points, index * block, block, 1)
        return jnp.dot(vector, matern(points, near), precision=highest)
    image = lax.map(rows_block, jnp.arange(total // block, dtype=jnp.int32))
    image = jnp.transpose(image, (1, 0, 2)).reshape(vector.shape[0], total)
    return image + vector

def reference(points, targets, order, landmarks):
    goal = jnp.take(targets, order, axis=1)
    anchors = jnp.take(points, landmarks, axis=1)
    cross = matern(points, anchors)
    gram = jnp.einsum('ni,nj->ij', cross, cross, precision=highest)
    count = anchors.shape[1]
    inner = matern(anchors, anchors) + jnp.eye(count, dtype=jnp.float32) + gram
    factor = jnp.linalg.cholesky(inner)

    def precondition(vector):
        summed = jnp.dot(vector, cross, precision=highest)
        weights = jax.scipy.linalg.cho_solve((factor, True), summed.T)
        return vector - jnp.dot(cross, weights, precision=highest).T
    solution = jnp.zeros_like(goal)
    residual = goal
    direction = goal
    previous = None
    for step in range(ITERS):
        scaled_res = precondition(residual)
        current = lax.optimization_barrier(jnp.sum(residual * scaled_res, axis=1))
        if step == 0:
            direction = scaled_res
        else:
            direction = scaled_res + (current / previous)[:, None] * direction
        image = operator(points, direction)
        stride = current / lax.optimization_barrier(jnp.sum(direction * image, axis=1))
        solution = solution + stride[:, None] * direction
        residual = residual - stride[:, None] * image
        previous = current
    return (solution, residual)
```

```python
import functools
import math

import jax
import jax.numpy as jnp
from jax import lax
from jax.experimental import pallas as pl
from jax.experimental.pallas import tpu as pltpu
from jax.sharding import PartitionSpec as P

ITERS = 2


root_five = 2.23606797749979
signal_var = 0.1
inverse_square_length = 25.0
highest = lax.Precision.HIGHEST

RESIDENT_POINTS = 2048
BLOCK = 256
LANES = 128
SUBLANES = 8


def matern(near, far):
    first = near[0][:, None] - far[0][None, :]
    second = near[1][:, None] - far[1][None, :]
    third = near[2][:, None] - far[2][None, :]
    scaled = (first * first + second * second + third * third) * inverse_square_length
    reach = jnp.sqrt(scaled)
    return signal_var * (1.0 + root_five * reach + 5.0 / 3.0 * scaled) * jnp.exp(-root_five * reach)


def tile_product(near, piece):
    width = piece.shape[1]
    block = math.gcd(width, 512)

    def accumulate(index, total):
        slab = lax.dynamic_slice_in_dim(piece, index * block, block, 1)
        return total + jnp.dot(slab[3:], matern(slab[:3], near), precision=highest)

    empty = jnp.zeros((piece.shape[0] - 3, near.shape[1]), jnp.float32)
    return lax.fori_loop(0, width // block, accumulate, empty)


def landmark_total(vector, cross):
    return lax.psum(jnp.dot(vector, cross, precision=highest), ("pts", "lm"))


def spread_body(points, targets, order, landmarks):
    rows = points.shape[1]
    count = landmarks.shape[0]
    offset = lax.axis_index(("pts", "lm")) * rows
    every = lax.all_gather(targets, ("pts", "lm"), axis=1, tiled=True)
    goal = jnp.take(every, order, axis=1)
    local = landmarks - offset
    inside = (local >= 0) & (local < rows)
    picked = jnp.where(inside[None, :], jnp.take(points, jnp.clip(local, 0, rows - 1), axis=1), 0.0)
    anchors = lax.psum(picked, ("pts", "lm"))
    cross = matern(points, anchors)
    gram = lax.psum(jnp.einsum("ri,rj->ij", cross, cross, precision=highest), ("pts", "lm"))
    inner = matern(anchors, anchors) + jnp.eye(count, dtype=jnp.float32) + gram
    factor = jnp.linalg.cholesky(inner)
    solution = jnp.zeros_like(goal)
    residual = goal
    summed = landmark_total(residual, cross)
    for step in range(ITERS):
        weights = jax.scipy.linalg.cho_solve((factor, True), summed.T)
        scaled_res = residual - jnp.dot(cross, weights, precision=highest).T
        stacked = jnp.concatenate([points, scaled_res], axis=0)
        image = (
            tile_product(points, lax.all_gather(stacked, ("pts", "lm"), axis=1, tiled=True))
            + scaled_res
        )
        current, curvature, lifted = lax.psum(
            (
                jnp.sum(residual * scaled_res, axis=1),
                jnp.sum(scaled_res * image, axis=1),
                jnp.dot(image, cross, precision=highest),
            ),
            ("pts", "lm"),
        )
        if step == 0:
            stride = current / curvature
            direction = scaled_res
            along = image
            along_lift = lifted
        else:
            ratio = current / previous
            stride = current / (curvature - ratio * current / stride)
            direction = scaled_res + ratio[:, None] * direction
            along = image + ratio[:, None] * along
            along_lift = lifted + ratio[:, None] * along_lift
        solution = solution + stride[:, None] * direction
        residual = residual - stride[:, None] * along
        summed = summed - stride[:, None] * along_lift
        previous = current
    return (solution, residual)


def split2(x):
    high = x.astype(jnp.bfloat16)
    low = (x - high.astype(jnp.float32)).astype(jnp.bfloat16)
    return high, low


def split3(x):
    high = x.astype(jnp.bfloat16)
    rest = x - high.astype(jnp.float32)
    mid = rest.astype(jnp.bfloat16)
    low = (rest - mid.astype(jnp.float32)).astype(jnp.bfloat16)
    return high, mid, low


def dot_nn(a, b):
    return lax.dot_general(a, b, (((1,), (0,)), ((), ())), preferred_element_type=jnp.float32)


def dot_nt(a, b):
    return lax.dot_general(a, b, (((1,), (1,)), ((), ())), preferred_element_type=jnp.float32)


def dot3(dot, ah, al, bh, bl):
    return dot(ah, bh) + (dot(ah, bl) + dot(al, bh))


def stack3(x):
    return jnp.concatenate(split3(x), axis=0)


def tall_dot(dot, rows, x3, high, low):
    one = dot(x3, high)
    two = dot(x3[: 2 * rows], low)
    return one[:rows] + (one[rows : 2 * rows] + two[:rows]) + (one[2 * rows :] + two[rows:])


def matern_tile(ax, ay, az, bx, by, bz):
    dx = ax - bx
    dy = ay - by
    dz = az - bz
    squared = dx * dx + dy * dy + dz * dz
    reach = squared * lax.rsqrt(jnp.maximum(squared, 1e-30))
    poly = signal_var + signal_var * reach + (signal_var / 3.0) * squared
    return poly * jnp.exp(-reach)


def whole_kernel(
    me_ref, g_ref, lm_ref, co_ref, re_ref,
    pts, goal, acols, pcols, arow, kh, kl, ch, cl, a_ref, ih, il, wh, wl, vec, lifted, wide,
):
    slots = g_ref.shape[0]
    rhs = co_ref.shape[0]
    n = slots * LANES
    m = lm_ref.shape[1]
    f32 = jnp.float32
    bf16 = jnp.bfloat16
    bits = slots.bit_length() - 1
    me = me_ref[0]

    def source(slot):
        out = 0
        for b in range(bits):
            if slot >> b & 1:
                out |= 1 << (bits - 1 - b)
        return jnp.bitwise_xor(me, out)

    scale = 5.0 * root_five
    for j in range(slots):
        at = pl.ds(j * LANES, LANES)
        pts[:, at] = g_ref[j, rhs : rhs + SUBLANES, :]

    marks = lm_ref[...]
    order = pts[3:4, :].astype(jnp.int32)
    anchor_sum = jnp.zeros((4 * SUBLANES, m), f32)
    for j in range(slots):
        ids = lax.broadcasted_iota(jnp.int32, (LANES, 1), 0) + source(j) * LANES
        hot = (ids == marks).astype(f32).astype(bf16)
        piece = g_ref[j, rhs : rhs + SUBLANES, :] * scale
        p3 = jnp.concatenate(split3(piece) + (jnp.zeros((SUBLANES, LANES), bf16),), axis=0)
        anchor_sum = anchor_sum + dot_nn(p3, hot)
    anchors = anchor_sum[:SUBLANES] + anchor_sum[SUBLANES : 2 * SUBLANES] + anchor_sum[2 * SUBLANES : 3 * SUBLANES]
    arow[...] = anchors
    acols[...] = anchors.T
    pts[...] = pts[...] * scale
    pcols[...] = pts[...].T

    goal3 = jnp.zeros((3 * rhs, n), f32)
    for j in range(slots):
        ids = lax.broadcasted_iota(jnp.int32, (LANES, 1), 0) + source(j) * LANES
        hot = (ids == order).astype(f32).astype(bf16)
        goal3 = goal3 + dot_nn(stack3(g_ref[j, :rhs, :]), hot)
    goal[...] = goal3[:rhs] + goal3[rhs : 2 * rhs] + goal3[2 * rhs :]

    chunk = 16
    lanes = 512

    def build(cols, row, width, store, per):
        def step(i, carry):
            for s in range(per):
                at = pl.multiple_of((i * per + s) * chunk, chunk)
                ax = cols[pl.ds(at, chunk), 0:1]
                ay = cols[pl.ds(at, chunk), 1:2]
                az = cols[pl.ds(at, chunk), 2:3]
                for l in range(0, width, lanes):
                    tile = matern_tile(
                        ax, ay, az, row[0:1, l : l + lanes], row[1:2, l : l + lanes], row[2:3, l : l + lanes]
                    )
                    store(at, l, tile)
            return carry

        lax.fori_loop(0, cols.shape[0] // (chunk * per), step, 0)

    def store_cross(at, l, tile):
        h, low = split2(tile)
        ch[pl.ds(at, chunk), l : l + lanes] = h
        cl[pl.ds(at, chunk), l : l + lanes] = low

    def store_kern(at, l, tile):
        h, low = split2(tile)
        kh[pl.ds(at, chunk), l : l + lanes] = h
        kl[pl.ds(at, chunk), l : l + lanes] = low

    def store_inner(at, l, tile):
        i = lax.broadcasted_iota(jnp.int32, (chunk, lanes), 0) + at
        k = lax.broadcasted_iota(jnp.int32, (chunk, lanes), 1) + l
        a_ref[pl.ds(at, chunk), l : l + lanes] = tile + jnp.where(i == k, 1.0, 0.0)

    build(acols, pts, n, store_cross, 2)
    build(acols, arow, m, store_inner, 4)
    build(pcols, pts, n, store_kern, 2)

    nb = m // BLOCK

    def blk(i):
        return pl.ds(i * BLOCK, BLOCK)

    for i in range(nb):
        for j in range(i + 1):
            a_ref[blk(i), blk(j)] += dot3(dot_nt, ch[blk(i), :], cl[blk(i), :], ch[blk(j), :], cl[blk(j), :])

    eye = (
        lax.broadcasted_iota(jnp.int32, (BLOCK, BLOCK), 0) == lax.broadcasted_iota(jnp.int32, (BLOCK, BLOCK), 1)
    ).astype(f32)
    for k in range(nb):
        d = a_ref[blk(k), blk(k)]
        top = jnp.max(jnp.sum(jnp.abs(d), axis=0, keepdims=True))
        c = 2.0 / (1.0 + top)
        rate = (top - 1.0) / (top + 1.0)
        power = eye - c * d
        vec[0:BLOCK, :] = c * (eye + power)
        vec[BLOCK : 2 * BLOCK, :] = power

        def refine(left):
            vh, vl = split2(vec[...])
            bh, bl = vh[BLOCK:], vl[BLOCK:]
            square = dot3(dot_nn, bh, bl, bh, bl)
            sh, sl = split2(square)
            vec[0:BLOCK, :] += dot3(dot_nn, vh[:BLOCK], vl[:BLOCK], sh, sl)
            vec[BLOCK : 2 * BLOCK, :] = square
            return left * left

        lax.while_loop(lambda left: left > 1e-4, refine, rate * rate)
        dh, dl = split2(d)
        x = vec[0:BLOCK, :]
        for _ in range(2):
            d3 = split3(d)
            x3 = split3(x)
            prod = (
                dot_nn(d3[0], x3[0])
                + (dot_nn(d3[0], x3[1]) + dot_nn(d3[1], x3[0]))
                + (dot_nn(d3[0], x3[2]) + dot_nn(d3[1], x3[1]) + dot_nn(d3[2], x3[0]))
            )
            err = eye - prod
            eh, el = split2(err)
            x = x + dot3(dot_nn, x3[0], x3[1], eh, el)
        xh, xl = split2(x)
        ih[k] = xh
        il[k] = xl
        if k + 1 < nb:
            panels = []
            for i in range(k + 1, nb):
                ph, plow = split2(a_ref[blk(i), blk(k)])
                w = dot3(dot_nn, ph, plow, xh, xl)
                h, low = split2(w)
                wh[blk(i), blk(k)] = h
                wl[blk(i), blk(k)] = low
                panels.append((ph, plow))
                for j in range(k + 1, i + 1):
                    qh, ql = panels[j - k - 1]
                    a_ref[blk(i), blk(j)] -= dot3(dot_nt, h, low, qh, ql)

    def inner_solve(u):
        parts = [u[:, i * BLOCK : (i + 1) * BLOCK] for i in range(nb)]
        for j in range(nb):
            y3 = stack3(parts[j])
            for i in range(j + 1, nb):
                parts[i] = parts[i] - tall_dot(dot_nt, rhs, y3, wh[blk(i), blk(j)], wl[blk(i), blk(j)])
            parts[j] = tall_dot(dot_nn, rhs, y3, ih[j], il[j])
        for i in range(nb - 1, 0, -1):
            y3 = stack3(parts[i])
            for j in range(i):
                parts[j] = parts[j] - tall_dot(dot_nn, rhs, y3, wh[blk(i), blk(j)], wl[blk(i), blk(j)])
        return jnp.concatenate(parts, axis=1)

    def product(dot, x, out, high, low, rows):
        x3 = stack3(x)

        def step(i, carry):
            at = pl.ds(pl.multiple_of(i * BLOCK, BLOCK), BLOCK)
            if rows:
                out[:, at] = tall_dot(dot, rhs, x3, high[at, :], low[at, :])
            else:
                out[:, at] = tall_dot(dot, rhs, x3, high[:, at], low[:, at])
            return carry

        lax.fori_loop(0, out.shape[1] // BLOCK, step, 0)

    residual = goal[...]
    coefficients = jnp.zeros_like(residual)
    for step in range(ITERS):
        product(dot_nt, residual, lifted, ch, cl, True)
        w = inner_solve(lifted[...])
        product(dot_nn, w, wide, ch, cl, False)
        z = residual - wide[...]
        gamma = jnp.sum(residual * z, axis=1, keepdims=True)
        if step == 0:
            direction = z
        else:
            direction = z + (gamma / previous) * direction
        product(dot_nn, direction, wide, kh, kl, False)
        image = direction + wide[...]
        alpha = gamma / jnp.sum(direction * image, axis=1, keepdims=True)
        coefficients = coefficients + alpha * direction
        residual = residual - alpha * image
        previous = gamma
    co_ref[...] = coefficients[:, :LANES]
    re_ref[...] = residual[:, :LANES]


def whole_body(shards, points, targets, order, landmarks):
    rows = points.shape[1]
    rhs = targets.shape[0]
    count = landmarks.shape[0]
    me = lax.axis_index(("pts", "lm"))
    pad = jnp.zeros((SUBLANES - 4, rows), jnp.float32)
    buffer = jnp.concatenate([targets, points, order.astype(jnp.float32)[None, :], pad], axis=0)[None]
    distance = shards // 2
    while distance:
        moved = lax.ppermute(buffer, ("pts", "lm"), [(i, i ^ distance) for i in range(shards)])
        buffer = jnp.concatenate([buffer, moved], axis=0)
        distance //= 2
    n = shards * rows
    vmem = pl.BlockSpec(memory_space=pltpu.VMEM)
    f32, bf16 = jnp.float32, jnp.bfloat16
    nb = count // BLOCK
    return pl.pallas_call(
        whole_kernel,
        name="whole",
        out_shape=(
            jax.ShapeDtypeStruct((rhs, rows), f32),
            jax.ShapeDtypeStruct((rhs, rows), f32),
        ),
        in_specs=[pl.BlockSpec(memory_space=pltpu.SMEM), vmem, vmem],
        out_specs=(vmem, vmem),
        scratch_shapes=[
            pltpu.VMEM((SUBLANES, n), f32),
            pltpu.VMEM((rhs, n), f32),
            pltpu.VMEM((count, SUBLANES), f32),
            pltpu.VMEM((n, SUBLANES), f32),
            pltpu.VMEM((SUBLANES, count), f32),
            pltpu.VMEM((n, n), bf16),
            pltpu.VMEM((n, n), bf16),
            pltpu.VMEM((count, n), bf16),
            pltpu.VMEM((count, n), bf16),
            pltpu.VMEM((count, count), f32),
            pltpu.VMEM((nb, BLOCK, BLOCK), bf16),
            pltpu.VMEM((nb, BLOCK, BLOCK), bf16),
            pltpu.VMEM((count, count), bf16),
            pltpu.VMEM((count, count), bf16),
            pltpu.VMEM((2 * BLOCK, BLOCK), f32),
            pltpu.VMEM((rhs, count), f32),
            pltpu.VMEM((rhs, n), f32),
        ],
        compiler_params=pltpu.CompilerParams(vmem_limit_bytes=60 * 1024 * 1024),
    )(me[None].astype(jnp.int32), buffer, landmarks[None, :])


def solution(mesh):
    shards = mesh.shape["pts"] * mesh.shape["lm"]

    def body(points, targets, order, landmarks):
        rows = points.shape[1]
        fits = (
            shards * rows <= RESIDENT_POINTS
            and shards & (shards - 1) == 0
            and rows == LANES
            and landmarks.shape[0] % BLOCK == 0
        )
        if fits:
            return whole_body(shards, points, targets, order, landmarks)
        return spread_body(points, targets, order, landmarks)

    return jax.shard_map(
        body,
        mesh=mesh,
        in_specs=(
            P(None, ("groups", "pts", "lm")),
            P(None, ("groups", "pts", "lm")),
            P(("groups", "pts", "lm")),
            P("groups"),
        ),
        out_specs=(P(None, ("groups", "pts", "lm")), P(None, ("groups", "pts", "lm"))),
        check_vma=False,
    )
```

```python
import functools
import math

import jax
import jax.numpy as jnp
from jax import lax
from jax.experimental import pallas as pl
from jax.experimental.pallas import tpu as pltpu
from jax.sharding import PartitionSpec as P

ITERS = 2


root_five = 2.23606797749979
signal_var = 0.1
inverse_square_length = 25.0
highest = lax.Precision.HIGHEST

RESIDENT_POINTS = 2048
BLOCK = 256
LANES = 128
SUBLANES = 8


def matern(near, far):
    first = near[0][:, None] - far[0][None, :]
    second = near[1][:, None] - far[1][None, :]
    third = near[2][:, None] - far[2][None, :]
    scaled = (first * first + second * second + third * third) * inverse_square_length
    reach = jnp.sqrt(scaled)
    return signal_var * (1.0 + root_five * reach + 5.0 / 3.0 * scaled) * jnp.exp(-root_five * reach)


def tile_product(near, piece):
    width = piece.shape[1]
    block = math.gcd(width, 512)

    def accumulate(index, total):
        slab = lax.dynamic_slice_in_dim(piece, index * block, block, 1)
        return total + jnp.dot(slab[3:], matern(slab[:3], near), precision=highest)

    empty = jnp.zeros((piece.shape[0] - 3, near.shape[1]), jnp.float32)
    return lax.fori_loop(0, width // block, accumulate, empty)


def landmark_total(vector, cross):
    return lax.psum(jnp.dot(vector, cross, precision=highest), ("pts", "lm"))


def spread_body(points, targets, order, landmarks):
    rows = points.shape[1]
    count = landmarks.shape[0]
    offset = lax.axis_index(("pts", "lm")) * rows
    every = lax.all_gather(targets, ("pts", "lm"), axis=1, tiled=True)
    goal = jnp.take(every, order, axis=1)
    local = landmarks - offset
    inside = (local >= 0) & (local < rows)
    picked = jnp.where(inside[None, :], jnp.take(points, jnp.clip(local, 0, rows - 1), axis=1), 0.0)
    anchors = lax.psum(picked, ("pts", "lm"))
    cross = matern(points, anchors)
    gram = lax.psum(jnp.einsum("ri,rj->ij", cross, cross, precision=highest), ("pts", "lm"))
    inner = matern(anchors, anchors) + jnp.eye(count, dtype=jnp.float32) + gram
    factor = jnp.linalg.cholesky(inner)
    solution = jnp.zeros_like(goal)
    residual = goal
    summed = landmark_total(residual, cross)
    for step in range(ITERS):
        weights = jax.scipy.linalg.cho_solve((factor, True), summed.T)
        scaled_res = residual - jnp.dot(cross, weights, precision=highest).T
        stacked = jnp.concatenate([points, scaled_res], axis=0)
        image = (
            tile_product(points, lax.all_gather(stacked, ("pts", "lm"), axis=1, tiled=True))
            + scaled_res
        )
        current, curvature, lifted = lax.psum(
            (
                jnp.sum(residual * scaled_res, axis=1),
                jnp.sum(scaled_res * image, axis=1),
                jnp.dot(image, cross, precision=highest),
            ),
            ("pts", "lm"),
        )
        if step == 0:
            stride = current / curvature
            direction = scaled_res
            along = image
            along_lift = lifted
        else:
            ratio = current / previous
            stride = current / (curvature - ratio * current / stride)
            direction = scaled_res + ratio[:, None] * direction
            along = image + ratio[:, None] * along
            along_lift = lifted + ratio[:, None] * along_lift
        solution = solution + stride[:, None] * direction
        residual = residual - stride[:, None] * along
        summed = summed - stride[:, None] * along_lift
        previous = current
    return (solution, residual)


def split2(x):
    high = x.astype(jnp.bfloat16)
    low = (x - high.astype(jnp.float32)).astype(jnp.bfloat16)
    return high, low


def split3(x):
    high = x.astype(jnp.bfloat16)
    rest = x - high.astype(jnp.float32)
    mid = rest.astype(jnp.bfloat16)
    low = (rest - mid.astype(jnp.float32)).astype(jnp.bfloat16)
    return high, mid, low


def dot_nn(a, b):
    return lax.dot_general(a, b, (((1,), (0,)), ((), ())), preferred_element_type=jnp.float32)


def dot_nt(a, b):
    return lax.dot_general(a, b, (((1,), (1,)), ((), ())), preferred_element_type=jnp.float32)


def dot3(dot, ah, al, bh, bl):
    return dot(ah, bh) + (dot(ah, bl) + dot(al, bh))


def stack3(x):
    return jnp.concatenate(split3(x), axis=0)


def tall_dot(dot, rows, x3, high, low):
    one = dot(x3, high)
    two = dot(x3[: 2 * rows], low)
    return one[:rows] + (one[rows : 2 * rows] + two[:rows]) + (one[2 * rows :] + two[rows:])


def matern_tile(ax, ay, az, bx, by, bz):
    dx = ax - bx
    dy = ay - by
    dz = az - bz
    squared = dx * dx + dy * dy + dz * dz
    reach = squared * lax.rsqrt(jnp.maximum(squared, 1e-30))
    poly = signal_var + signal_var * reach + (signal_var / 3.0) * squared
    return poly * jnp.exp(-reach)


def whole_kernel(
    me_ref, g_ref, lm_ref, co_ref, re_ref,
    pts, goal, acols, pcols, arow, kh, kl, ch, cl, a_ref, ih, il, wh, wl, vec, lifted, wide,
):
    slots = g_ref.shape[0]
    rhs = co_ref.shape[0]
    n = slots * LANES
    m = lm_ref.shape[1]
    f32 = jnp.float32
    bf16 = jnp.bfloat16
    bits = slots.bit_length() - 1
    me = me_ref[0]

    def source(slot):
        out = 0
        for b in range(bits):
            if slot >> b & 1:
                out |= 1 << (bits - 1 - b)
        return jnp.bitwise_xor(me, out)

    scale = 5.0 * root_five
    for j in range(slots):
        at = pl.ds(j * LANES, LANES)
        pts[:, at] = g_ref[j, rhs : rhs + SUBLANES, :]

    marks = lm_ref[...]
    order = pts[3:4, :].astype(jnp.int32)
    anchor_sum = jnp.zeros((4 * SUBLANES, m), f32)
    for j in range(slots):
        ids = lax.broadcasted_iota(jnp.int32, (LANES, 1), 0) + source(j) * LANES
        hot = (ids == marks).astype(f32).astype(bf16)
        piece = g_ref[j, rhs : rhs + SUBLANES, :] * scale
        p3 = jnp.concatenate(split3(piece) + (jnp.zeros((SUBLANES, LANES), bf16),), axis=0)
        anchor_sum = anchor_sum + dot_nn(p3, hot)
    anchors = anchor_sum[:SUBLANES] + anchor_sum[SUBLANES : 2 * SUBLANES] + anchor_sum[2 * SUBLANES : 3 * SUBLANES]
    arow[...] = anchors
    acols[...] = anchors.T
    pts[...] = pts[...] * scale
    pcols[...] = pts[...].T

    goal3 = jnp.zeros((3 * rhs, n), f32)
    for j in range(slots):
        ids = lax.broadcasted_iota(jnp.int32, (LANES, 1), 0) + source(j) * LANES
        hot = (ids == order).astype(f32).astype(bf16)
        goal3 = goal3 + dot_nn(stack3(g_ref[j, :rhs, :]), hot)
    goal[...] = goal3[:rhs] + goal3[rhs : 2 * rhs] + goal3[2 * rhs :]

    chunk = 16
    lanes = 512

    def build(cols, row, width, store, per):
        def step(i, carry):
            for s in range(per):
                at = pl.multiple_of((i * per + s) * chunk, chunk)
                ax = cols[pl.ds(at, chunk), 0:1]
                ay = cols[pl.ds(at, chunk), 1:2]
                az = cols[pl.ds(at, chunk), 2:3]
                for l in range(0, width, lanes):
                    tile = matern_tile(
                        ax, ay, az, row[0:1, l : l + lanes], row[1:2, l : l + lanes], row[2:3, l : l + lanes]
                    )
                    store(at, l, tile)
            return carry

        lax.fori_loop(0, cols.shape[0] // (chunk * per), step, 0)

    def store_cross(at, l, tile):
        h, low = split2(tile)
        ch[pl.ds(at, chunk), l : l + lanes] = h
        cl[pl.ds(at, chunk), l : l + lanes] = low

    build(acols, pts, n, store_cross, 2)

    nb = m // BLOCK
    nbn = n // BLOCK
    inner_tiles = nb * (nb + 1) // 2
    kern_tiles = nbn * (nbn + 1) // 2
    per = -(-kern_tiles // inner_tiles)
    eye = (
        lax.broadcasted_iota(jnp.int32, (BLOCK, BLOCK), 0) == lax.broadcasted_iota(jnp.int32, (BLOCK, BLOCK), 1)
    ).astype(f32)

    def blk(i):
        return pl.ds(i * BLOCK, BLOCK)

    def dyn(i):
        return pl.ds(pl.multiple_of(i * BLOCK, BLOCK), BLOCK)

    def lower(t, count):
        i = 0
        for k in range(1, count):
            i = i + jnp.where(t >= k * (k + 1) // 2, 1, 0)
        return i, t - i * (i + 1) // 2

    def tile_rows(cols, i, row, j):
        far = [row[c : c + 1, dyn(j)] for c in range(3)]
        for s in range(0, BLOCK, chunk):
            at = pl.ds(pl.multiple_of(i * BLOCK + s, chunk), chunk)
            near = [cols[at, c : c + 1] for c in range(3)]
            yield s, at, matern_tile(*near, *far)

    def both(t, carry):
        i, j = lower(t, nb)
        gram = dot3(dot_nt, ch[dyn(i), :], cl[dyn(i), :], ch[dyn(j), :], cl[dyn(j), :])
        same = jnp.where(i == j, 1.0, 0.0)
        for s in range(per):
            ki, kj = lower(jnp.minimum(t * per + s, kern_tiles - 1), nbn)
            for _, at, tile in tile_rows(pcols, ki, pts, kj):
                h, low = split2(tile)
                kh[at, dyn(kj)] = h
                kl[at, dyn(kj)] = low
            kh[dyn(kj), dyn(ki)] = kh[dyn(ki), dyn(kj)].T
            kl[dyn(kj), dyn(ki)] = kl[dyn(ki), dyn(kj)].T
        for s, at, tile in tile_rows(acols, i, arow, j):
            part = slice(s, s + chunk)
            a_ref[at, dyn(j)] = gram[part] + tile + same * eye[part]
        return carry

    lax.fori_loop(0, inner_tiles, both, 0)

    for k in range(nb):
        d = a_ref[blk(k), blk(k)]
        top = jnp.max(jnp.sum(jnp.abs(d), axis=0, keepdims=True))
        c = 2.0 / (1.0 + top)
        rate = (top - 1.0) / (top + 1.0)
        vec[0:BLOCK, :] = c * eye
        vec[BLOCK : 2 * BLOCK, :] = eye - c * d

        def refine(left):
            s = 2.0 / (2.0 - left * left)
            vh, vl = split2(vec[...])
            both = dot3(dot_nn, vh, vl, vh[BLOCK:], vl[BLOCK:])
            vec[0:BLOCK, :] = s * (vec[0:BLOCK, :] + both[:BLOCK])
            vec[BLOCK : 2 * BLOCK, :] = (1.0 - s) * eye + s * both[BLOCK:]
            return s - 1.0

        lax.while_loop(lambda left: left > 3e-4, refine, rate)
        x = vec[0:BLOCK, :]
        d3 = split3(d)
        x3 = split3(x)
        prod = (
            dot_nn(d3[0], x3[0])
            + (dot_nn(d3[0], x3[1]) + dot_nn(d3[1], x3[0]))
            + (dot_nn(d3[0], x3[2]) + dot_nn(d3[1], x3[1]) + dot_nn(d3[2], x3[0]))
        )
        eh, el = split2(eye - prod)
        x = x + dot3(dot_nn, x3[0], x3[1], eh, el)
        xh, xl = split2(x)
        ih[k] = xh
        il[k] = xl
        if k + 1 < nb:
            panels = []
            for i in range(k + 1, nb):
                ph, plow = split2(a_ref[blk(i), blk(k)])
                w = dot3(dot_nn, ph, plow, xh, xl)
                h, low = split2(w)
                wh[blk(i), blk(k)] = h
                wl[blk(i), blk(k)] = low
                panels.append((ph, plow))
                for j in range(k + 1, i + 1):
                    qh, ql = panels[j - k - 1]
                    a_ref[blk(i), blk(j)] -= dot3(dot_nt, h, low, qh, ql)

    def inner_solve(u):
        parts = [u[:, i * BLOCK : (i + 1) * BLOCK] for i in range(nb)]
        for j in range(nb):
            y3 = stack3(parts[j])
            for i in range(j + 1, nb):
                parts[i] = parts[i] - tall_dot(dot_nt, rhs, y3, wh[blk(i), blk(j)], wl[blk(i), blk(j)])
            parts[j] = tall_dot(dot_nn, rhs, y3, ih[j], il[j])
        for i in range(nb - 1, 0, -1):
            y3 = stack3(parts[i])
            for j in range(i):
                parts[j] = parts[j] - tall_dot(dot_nn, rhs, y3, wh[blk(i), blk(j)], wl[blk(i), blk(j)])
        return jnp.concatenate(parts, axis=1)

    def product(dot, x, out, high, low, rows):
        x3 = stack3(x)

        for i in range(out.shape[1] // BLOCK):
            at = pl.ds(i * BLOCK, BLOCK)
            if rows:
                out[:, at] = tall_dot(dot, rhs, x3, high[at, :], low[at, :])
            else:
                out[:, at] = tall_dot(dot, rhs, x3, high[:, at], low[:, at])

    residual = goal[...]
    coefficients = jnp.zeros_like(residual)
    for step in range(ITERS):
        product(dot_nt, residual, lifted, ch, cl, True)
        w = inner_solve(lifted[...])
        product(dot_nn, w, wide, ch, cl, False)
        z = residual - wide[...]
        gamma = jnp.sum(residual * z, axis=1, keepdims=True)
        if step == 0:
            direction = z
        else:
            direction = z + (gamma / previous) * direction
        product(dot_nn, direction, wide, kh, kl, False)
        image = direction + wide[...]
        alpha = gamma / jnp.sum(direction * image, axis=1, keepdims=True)
        coefficients = coefficients + alpha * direction
        residual = residual - alpha * image
        previous = gamma
    co_ref[...] = coefficients[:, :LANES]
    re_ref[...] = residual[:, :LANES]


def whole_body(shards, points, targets, order, landmarks):
    rows = points.shape[1]
    rhs = targets.shape[0]
    count = landmarks.shape[0]
    me = lax.axis_index(("pts", "lm"))
    pad = jnp.zeros((SUBLANES - 4, rows), jnp.float32)
    buffer = jnp.concatenate([targets, points, order.astype(jnp.float32)[None, :], pad], axis=0)[None]
    distance = shards // 2
    while distance:
        moved = lax.ppermute(buffer, ("pts", "lm"), [(i, i ^ distance) for i in range(shards)])
        buffer = jnp.concatenate([buffer, moved], axis=0)
        distance //= 2
    n = shards * rows
    vmem = pl.BlockSpec(memory_space=pltpu.VMEM)
    f32, bf16 = jnp.float32, jnp.bfloat16
    nb = count // BLOCK
    return pl.pallas_call(
        whole_kernel,
        name="whole",
        out_shape=(
            jax.ShapeDtypeStruct((rhs, rows), f32),
            jax.ShapeDtypeStruct((rhs, rows), f32),
        ),
        in_specs=[pl.BlockSpec(memory_space=pltpu.SMEM), vmem, vmem],
        out_specs=(vmem, vmem),
        scratch_shapes=[
            pltpu.VMEM((SUBLANES, n), f32),
            pltpu.VMEM((rhs, n), f32),
            pltpu.VMEM((count, SUBLANES), f32),
            pltpu.VMEM((n, SUBLANES), f32),
            pltpu.VMEM((SUBLANES, count), f32),
            pltpu.VMEM((n, n), bf16),
            pltpu.VMEM((n, n), bf16),
            pltpu.VMEM((count, n), bf16),
            pltpu.VMEM((count, n), bf16),
            pltpu.VMEM((count, count), f32),
            pltpu.VMEM((nb, BLOCK, BLOCK), bf16),
            pltpu.VMEM((nb, BLOCK, BLOCK), bf16),
            pltpu.VMEM((count, count), bf16),
            pltpu.VMEM((count, count), bf16),
            pltpu.VMEM((2 * BLOCK, BLOCK), f32),
            pltpu.VMEM((rhs, count), f32),
            pltpu.VMEM((rhs, n), f32),
        ],
        compiler_params=pltpu.CompilerParams(vmem_limit_bytes=60 * 1024 * 1024),
    )(me[None].astype(jnp.int32), buffer, landmarks[None, :])


def solution(mesh):
    shards = mesh.shape["pts"] * mesh.shape["lm"]

    def body(points, targets, order, landmarks):
        rows = points.shape[1]
        fits = (
            shards * rows <= RESIDENT_POINTS
            and shards & (shards - 1) == 0
            and rows == LANES
            and landmarks.shape[0] % BLOCK == 0
        )
        if fits:
            return whole_body(shards, points, targets, order, landmarks)
        return spread_body(points, targets, order, landmarks)

    return jax.shard_map(
        body,
        mesh=mesh,
        in_specs=(
            P(None, ("groups", "pts", "lm")),
            P(None, ("groups", "pts", "lm")),
            P(("groups", "pts", "lm")),
            P("groups"),
        ),
        out_specs=(P(None, ("groups", "pts", "lm")), P(None, ("groups", "pts", "lm"))),
        check_vma=False,
    )
```
